32 devices in a mesh: level: 2 (over x), subj: 4 (over y, core), gz: 4 (over z).
Axes of the slice: x: 2, y: 2, z: 4, core: 2. Of those that a mesh axis runs over, the one named last changes fastest.
Arguments:
- images: bfloat16 [8, 192, 192, 192], P('subj', 'gz'), may hold values from -6 to 6
- momenta: float32 [8, 96, 3, 96, 96], P('subj', 'gz'), may hold values from -18 to 18
- assign: int32 [8], replicated, may hold values from 0 to 7, as said below
Outputs:
- template: float32 [192, 192, 192], P('gz')
The draws below stay inside these ranges and needn't reach their ends.
Inputs may be any that keep to these rules, and one draw needn't show every extreme that they name: assign is a permutation of 0 to 7 with assign[i] % 2 == i % 2 for every i.
All inputs are finite; a program needn't handle non-finite values.
Results may differ from the reference program's by a relative error of at most 0.00069.
Values may be sent and summed in bfloat16 or wider, within the bound.
A program may use at most 128 MiB of HBM per device.

```python
import jax
import jax.numpy as jnp
from jax import lax

NF = 192
NC = 96
SUBJ_DEV = 2
SWEEPS = 2
SUBJECTS = 8


def draw_assign(key, part):
    groups = SUBJECTS // SUBJ_DEV
    keys = jax.random.split(jax.random.fold_in(key, 7), SUBJ_DEV)
    orders = jax.vmap(lambda single: jax.random.permutation(single, groups))(keys)
    slots = jnp.arange(SUBJ_DEV, dtype=jnp.int32)
    table = orders.T.astype(jnp.int32) * SUBJ_DEV + slots[None, :]
    return table.reshape(SUBJECTS)


def block_levels(stream_key, dims, cuts, smallest, largest):
    level, own = 1.0, jax.random.fold_in(stream_key, 6)
    for position, parts in cuts:
        draws = jnp.exp(jax.random.uniform(jax.random.fold_in(own, position), (parts,), jnp.float32, smallest / len(cuts), largest / len(cuts)))
        level = level * jnp.repeat(draws, dims[position] // parts).reshape([-1 if axis == position else 1 for axis in range(len(dims))])
    return level


def bell_draw(stream_key, extent, deviation, limit, cuts=(), kind=jnp.bfloat16):
    entries = jax.random.normal(stream_key, extent, jnp.float32) * deviation
    if len(cuts) > 0:
        entries = block_levels(stream_key, extent, cuts, -0.22, 0.18) * entries
    return jnp.clip(entries, min=-limit, max=limit).astype(kind)


def setup_inputs(seed: int = 0) -> dict:
    key_of = jax.random.split(jax.random.key(seed), 4)
    return {
        "images": bell_draw(key_of[0], (SUBJECTS, NF, NF, NF), 1.0, 6.0, ((0, 4), (1, 4))),
        "momenta": bell_draw(key_of[1], (SUBJECTS, NC, 3, NC, NC), 3.0, 18.0, ((0, 4), (1, 4)), jnp.float32),
        "assign": draw_assign(jax.random.fold_in(key_of[3], 71), 0),
    }


def band(padded, count, axis):
    def take(offset):
        return lax.slice_in_dim(padded, offset, offset + count, axis=axis)
    return (take(0) + take(4)) * 0.0625 + (take(1) + take(3)) * 0.25 + take(2) * 0.375


def blur_plane(field, axis):
    widths = [(2, 2) if dimension == axis else (0, 0) for dimension in range(field.ndim)]
    return band(jnp.pad(field, widths), field.shape[axis], axis)


def upsample_table(finest, coarse, offset):
    rows_fine = jnp.arange(finest, dtype=jnp.int32)[:, None]
    columns = jnp.arange(coarse, dtype=jnp.int32)[None, :]
    nearest = rows_fine // 2 + offset
    farther = nearest + 2 * (rows_fine % 2) - 1
    return 0.75 * (columns == nearest).astype(jnp.float32) + 0.25 * (columns == farther).astype(jnp.float32)


def warp_slab(extended, upsampled):
    center = extended[1:-1]
    grad_z = (extended[2:] - extended[:-2]) * 0.5
    padded_y = jnp.pad(center, ((0, 0), (1, 1), (0, 0)))
    grad_y = (padded_y[:, 2:] - padded_y[:, :-2]) * 0.5
    padded_x = jnp.pad(center, ((0, 0), (0, 0), (1, 1)))
    grad_x = (padded_x[:, :, 2:] - padded_x[:, :, :-2]) * 0.5
    return center - (upsampled[:, 0] * grad_x + upsampled[:, 1] * grad_y + upsampled[:, 2] * grad_z)


def relax(extended):
    center = extended[1:-1]
    padded_y = jnp.pad(center, ((0, 0), (1, 1), (0, 0)))
    padded_x = jnp.pad(center, ((0, 0), (0, 0), (1, 1)))
    neighbours = extended[2:] + extended[:-2] + padded_y[:, 2:] + padded_y[:, :-2] + padded_x[:, :, 2:] + padded_x[:, :, :-2]
    return center + 0.15 * (neighbours - 6.0 * center)


def reference(images, momenta, assign):
    table = upsample_table(NF, NC, 0)
    highest = lax.Precision.HIGHEST

    def per_subject(total, element):
        image, source = element
        moment = lax.dynamic_index_in_dim(momenta, source, 0, keepdims=False)
        smooth = blur_plane(blur_plane(blur_plane(moment, 3), 2), 0)
        coarse_field = smooth.astype(jnp.bfloat16).astype(jnp.float32)
        section_x = jnp.einsum('zcyx,Xx->zcyX', coarse_field, table, precision=highest)
        section_y = jnp.einsum('zcyX,Yy->zcYX', section_x, table, precision=highest)
        upsampled = jnp.einsum('zcYX,Zz->ZcYX', section_y, table, precision=highest)
        extended = jnp.pad(image.astype(jnp.float32), ((1, 1), (0, 0), (0, 0)))
        return total + warp_slab(extended, upsampled), None

    start_total = jnp.zeros((NF, NF, NF), jnp.float32)
    total, _ = lax.scan(per_subject, start_total, (images, assign))
    mean = total / SUBJECTS
    for repeat in range(SWEEPS):
        mean = relax(jnp.pad(mean, ((1, 1), (0, 0), (0, 0))))
    return mean
```

```python
import jax
import jax.numpy as jnp
from jax import lax
from jax.experimental import pallas as pl
from jax.experimental.pallas import tpu as pltpu
from jax.sharding import PartitionSpec as P

SWEEPS = 2


def with_halo(array, sides, width):
    for axis, dim in sides:
        size, length = (lax.axis_size(axis), array.shape[dim])
        up = [(i, (i + 1) % size) for i in range(size - 1)]
        down = [(j, i) for i, j in up]
        last = lax.slice_in_dim(array, length - width, length, axis=dim)
        leading = lax.slice_in_dim(array, 0, width, axis=dim)
        before = lax.ppermute(last, axis, up)
        after = lax.ppermute(leading, axis, down)
        array = jnp.concatenate([before, array, after], axis=dim)
    return array


def band(padded, count, axis):

    def take(offset):
        return lax.slice_in_dim(padded, offset, offset + count, axis=axis)

    return (take(0) + take(4)) * 0.0625 + (take(1) + take(3)) * 0.25 + take(2) * 0.375


def blur_plane(field, axis):
    widths = [(2, 2) if dimension == axis else (0, 0) for dimension in range(field.ndim)]
    return band(jnp.pad(field, widths), field.shape[axis], axis)


def upsample_table(finest, coarse, offset):
    rows_fine = jnp.arange(finest, dtype=jnp.int32)[:, None]
    columns = jnp.arange(coarse, dtype=jnp.int32)[None, :]
    nearest = rows_fine // 2 + offset
    farther = nearest + 2 * (rows_fine % 2) - 1
    return 0.75 * (columns == nearest).astype(jnp.float32) + 0.25 * (columns == farther).astype(
        jnp.float32
    )


def halo_rows(first, last, axis):
    size = lax.axis_size(axis)
    up = [(i, (i + 1) % size) for i in range(size - 1)]
    down = [(j, i) for i, j in up]
    return lax.ppermute(last, axis, up), lax.ppermute(first, axis, down)


def slope_table(finest):
    rows = jnp.arange(finest, dtype=jnp.int32)[:, None]
    columns = jnp.arange(finest, dtype=jnp.int32)[None, :]
    ahead = (columns == rows + 1).astype(jnp.float32)
    behind = (columns == rows - 1).astype(jnp.float32)
    return ((ahead - behind) * 0.5).astype(jnp.bfloat16)


LANES = 128


def pack_coarse(field):
    coarse = field.shape[-1]
    rest = LANES - coarse
    kept = coarse * coarse // LANES
    tail = field[..., kept:, :]
    pieces = [tail[..., i : i + rest] for i in range(0, coarse, rest)]
    return jnp.concatenate([field[..., :kept, :], jnp.concatenate(pieces, axis=-2)], axis=-1)


def warp_kernel(
    sel, velocity, pair, below, above, before, after, up_x, up_y, slope_x, slope_y, out, fine
):
    step = pl.program_id(0)
    last = pl.num_programs(0) - 1
    for c in range(3):
        packed = velocity[0, 0, c]
        parts = [
            jnp.dot(packed, up_x[i], preferred_element_type=jnp.float32)
            for i in range(up_x.shape[0])
        ]
        size = packed.shape[0] // (len(parts) - 1)
        tail = parts[1][:size]
        for i in range(2, len(parts)):
            tail = tail + parts[i][(i - 1) * size : i * size]
        wide = jnp.concatenate([parts[0], tail], axis=0)
        high = wide.astype(jnp.bfloat16)
        low = (wide - high.astype(jnp.float32)).astype(jnp.bfloat16)
        both = jnp.concatenate([high, low], axis=0)
        fine[lax.rem(step, 3), c] = jnp.dot(up_y[...], both, preferred_element_type=jnp.float32)

    @pl.when(step >= 2)
    def _():
        finest = pair.shape[2]
        half = finest // 2
        rest = finest - LANES
        chunk = finest // 4
        scale = sel[2].astype(jnp.float32) * (1.0 / sel[3].astype(jnp.float32))
        middle = lax.rem(step + 2, 3)
        prior_is_halo = step == 2
        next_is_halo = step == last
        for z in range(2):
            outer = lax.rem(step + 1, 3) if z == 0 else lax.rem(step, 3)
            for r in range(0, finest, chunk):
                rows = pl.ds(r, chunk)
                image = pair[0, z, rows, :]
                dx = jnp.dot(image, slope_x[...], preferred_element_type=jnp.float32)
                dy = jnp.dot(
                    slope_y[rows, :], pair[0, z], preferred_element_type=jnp.float32
                )
                if z == 0:
                    back = jnp.where(
                        prior_is_halo,
                        before[0, rows, :].astype(jnp.float32),
                        below[0, 0, rows, :].astype(jnp.float32),
                    )
                    ahead = pair[0, 1, rows, :].astype(jnp.float32)
                else:
                    back = pair[0, 0, rows, :].astype(jnp.float32)
                    ahead = jnp.where(
                        next_is_halo,
                        after[0, rows, :].astype(jnp.float32),
                        above[0, 0, rows, :].astype(jnp.float32),
                    )
                dz = (ahead - back) * 0.5
                near = (
                    fine[middle, 0, rows, :] * dx
                    + fine[middle, 1, rows, :] * dy
                    + fine[middle, 2, rows, :] * dz
                )
                far = (
                    fine[outer, 0, rows, :] * dx
                    + fine[outer, 1, rows, :] * dy
                    + fine[outer, 2, rows, :] * dz
                )
                value = scale * (image.astype(jnp.float32) - (0.75 * near + 0.25 * far))
                out[z, rows, :] = value[:, :LANES]
                side = rest * (r // half)
                out[z, pl.ds(finest + r % half, chunk), side : side + rest] = value[:, LANES:]


def warp(sel, gathered, images, before, after, interpret=False):
    finest = images.shape[2]
    slab_ext, kept = gathered.shape[1], gathered.shape[3]
    coarse = finest // 2
    rest = LANES - coarse
    fine_slab = images.shape[1]
    table = upsample_table(finest, coarse, 0).astype(jnp.bfloat16)
    columns = table.T
    up_x = [jnp.pad(columns, ((0, rest), (0, 0)))]
    for i in range(0, coarse, rest):
        up_x.append(jnp.pad(columns[i : i + rest], ((coarse, 0), (0, 0))))
    up_x = jnp.stack(up_x)
    slope = slope_table(finest)
    whole = lambda j, s: (0, 0)
    edge = lambda j, s: (0, 0, 0)
    lag = lambda j: jnp.maximum(j - 2, 0)
    plane = (1, 1, finest, finest)
    grid_spec = pltpu.PrefetchScalarGridSpec(
        num_scalar_prefetch=1,
        grid=(slab_ext,),
        in_specs=[
            pl.BlockSpec((1, 1, 3, kept, LANES), lambda j, s: (s[1], j, 0, 0, 0)),
            pl.BlockSpec((1, 2, finest, finest), lambda j, s: (s[0], lag(j), 0, 0)),
            pl.BlockSpec(plane, lambda j, s: (s[0], jnp.maximum(2 * lag(j) - 1, 0), 0, 0)),
            pl.BlockSpec(
                plane, lambda j, s: (s[0], jnp.minimum(2 * lag(j) + 2, fine_slab - 1), 0, 0)
            ),
            pl.BlockSpec((1, finest, finest), edge),
            pl.BlockSpec((1, finest, finest), edge),
            pl.BlockSpec(up_x.shape, edge),
            pl.BlockSpec((finest, 2 * coarse), whole),
            pl.BlockSpec((finest, finest), whole),
            pl.BlockSpec((finest, finest), whole),
        ],
        out_specs=pl.BlockSpec(
            (2, finest + finest // 2, LANES), lambda j, s: (lag(j), 0, 0)
        ),
        scratch_shapes=[pltpu.VMEM((3, 3, finest, finest), jnp.float32)],
    )
    return pl.pallas_call(
        warp_kernel,
        grid_spec=grid_spec,
        out_shape=jax.ShapeDtypeStruct((fine_slab, finest + finest // 2, LANES), jnp.float32),
        compiler_params=pltpu.CompilerParams(dimension_semantics=("arbitrary",)),
        interpret=interpret,
    )(
        sel,
        gathered,
        images,
        images,
        images,
        before,
        after,
        up_x,
        jnp.concatenate([table, table], axis=1),
        slope.T,
        slope,
    )


MARGIN = 8


def relax_row(ref, slot, behind, ahead, r, chunk):
    rows = pl.ds(MARGIN + r, chunk)
    center = ref[slot, rows, :]
    width = center.shape[1]
    neighbours = (
        ref[behind, rows, :]
        + ref[ahead, rows, :]
        + ref[slot, pl.ds(MARGIN + r - 1, chunk), :]
        + ref[slot, pl.ds(MARGIN + r + 1, chunk), :]
        + pltpu.roll(center, 1, 1)
        + pltpu.roll(center, width - 1, 1)
    )
    return center + 0.15 * (neighbours - 6.0 * center)


def sweep_kernel(sel, mean, before, after, out, first, second):
    step = pl.program_id(0)
    last = pl.num_programs(0) - 1
    finest = out.shape[1]
    half = finest // 2
    rest = finest - LANES
    chunk = finest // 3
    base = 2 * lax.rem(step, 2)
    other = 2 - base

    def enter(ref):
        for z in range(2):
            slot = base + z
            first[slot, pl.ds(MARGIN, finest), 0:LANES] = ref[z, 0:finest, :]
            side = ref[z, finest : finest + half, :]
            first[slot, pl.ds(MARGIN, half), LANES:finest] = side[:, :rest]
            turned = pltpu.roll(side, LANES - rest, 1)
            first[slot, pl.ds(MARGIN + half, half), LANES:finest] = turned[:, :rest]

    @pl.when(step == 0)
    def _():
        first[...] = jnp.zeros_like(first)
        second[...] = jnp.zeros_like(second)
        enter(before)

    @pl.when((step > 0) & (step < last))
    def _():
        enter(mean)

    @pl.when(step == last)
    def _():
        enter(after)

    @pl.when(step >= 1)
    def _():
        keep_low = jnp.where((step == 1) & (sel[0] == 0), 0.0, 1.0)
        keep_high = jnp.where((step == last) & (sel[0] == sel[1]), 0.0, 1.0)
        places = ((other + 1, other, base, keep_low), (base, other + 1, base + 1, keep_high))
        for slot, behind, ahead, keep in places:
            for r in range(0, finest, chunk):
                value = relax_row(first, slot, behind, ahead, r, chunk) * keep
                second[slot, pl.ds(MARGIN + r, chunk), 0:finest] = value[:, :finest]

    @pl.when(step >= 2)
    def _():
        places = ((other, base + 1, other + 1), (other + 1, other, base))
        for z, (slot, behind, ahead) in enumerate(places):
            for r in range(0, finest, chunk):
                value = relax_row(second, slot, behind, ahead, r, chunk)
                out[z, pl.ds(r, chunk), :] = value[:, :finest]


def sweeps(sel, mean, before, after, finest, interpret=False):
    fine_slab = mean.shape[0]
    blocks = fine_slab // 2
    block = (2,) + mean.shape[1:]
    width = -(-(finest + 1) // LANES) * LANES
    ring = pltpu.VMEM((4, finest + 2 * MARGIN, width), jnp.float32)
    grid_spec = pltpu.PrefetchScalarGridSpec(
        num_scalar_prefetch=1,
        grid=(blocks + 2,),
        in_specs=[
            pl.BlockSpec(block, lambda j, s: (jnp.clip(j - 1, 0, blocks - 1), 0, 0)),
            pl.BlockSpec(block, lambda j, s: (0, 0, 0)),
            pl.BlockSpec(block, lambda j, s: (0, 0, 0)),
        ],
        out_specs=pl.BlockSpec(
            (2, finest, finest), lambda j, s: (jnp.maximum(j - 2, 0), 0, 0)
        ),
        scratch_shapes=[ring, ring],
    )
    return pl.pallas_call(
        sweep_kernel,
        grid_spec=grid_spec,
        out_shape=jax.ShapeDtypeStruct((fine_slab, finest, finest), jnp.float32),
        compiler_params=pltpu.CompilerParams(dimension_semantics=("arbitrary",)),
        interpret=interpret,
    )(sel, mean, before, after)


def shards(images, momenta, assign):
    count = momenta.shape[0]
    slab = momenta.shape[1]
    coarse = momenta.shape[3]
    finest = images.shape[2]
    fine_slab = images.shape[1]
    level_index = lax.axis_index("level")
    group_index = lax.axis_index("subj")
    zone_index = lax.axis_index("gz")
    rim_width = 3
    ticker = 0 + level_index
    weight = (ticker < count).astype(jnp.int32)
    ticker = jnp.minimum(ticker, count - 1)
    moment = lax.dynamic_index_in_dim(momenta, ticker, 0, keepdims=False)
    extended = with_halo(moment, (("gz", 0),), rim_width)
    smooth = blur_plane(blur_plane(extended, 3), 2)
    field = band(smooth, extended.shape[0] - 4, 0)
    global_z = zone_index * slab - 1 + jnp.arange(field.shape[0], dtype=jnp.int32)
    inside = (global_z >= 0) & (global_z < slab * lax.axis_size("gz"))
    field = jnp.where(inside[:, None, None, None], field, 0.0)
    field = pack_coarse(field.astype(jnp.bfloat16))
    source = assign[group_index * count + ticker] // count
    piece = lax.all_gather(field[None], "subj", axis=0, tiled=True)
    rows = lax.dynamic_slice_in_dim(images, ticker, 1, 0)
    image_before, image_after = halo_rows(rows[0, :1], rows[0, fine_slab - 1 :], "gz")
    subjects = jnp.int32(lax.axis_size("subj") * count)
    sel = jnp.stack([ticker, source, weight, subjects]).astype(jnp.int32)
    total = warp(sel, piece, images, image_before, image_after)
    mean = lax.psum(total, ("level", "subj"))
    mean_before, mean_after = halo_rows(mean[:2], mean[fine_slab - 2 :], "gz")
    zones = jnp.stack([zone_index, lax.axis_size("gz") - 1]).astype(jnp.int32)
    return sweeps(zones, mean, mean_before, mean_after, finest)


def solution(mesh):
    return jax.shard_map(
        shards,
        mesh=mesh,
        in_specs=(P("subj", "gz", None, None), P("subj", "gz", None, None, None), P()),
        out_specs=P("gz", None, None),
        check_vma=False,
    )
```
